32 devices in a mesh: row: 4 (over y, x), col: 2 (over core), depth: 4 (over z).
Axes of the slice: x: 2, y: 2, z: 4, core: 2. Of those that a mesh axis runs over, the one named last changes fastest.
Arguments:
- a_cols: float32 [4096, 1024], P(('row', 'col')), may hold values from -16 to 24, as said below
- past_panels: float32 [4096, 2048], P(('row', 'col'), 'depth'), may hold values from -1 to 1
Outputs:
- factor: float32 [4096, 1024], P(('row', 'col'))
The draws below stay inside these ranges and needn't reach their ends.
Inputs may be any that keep to these rules, and one draw needn't show every extreme that they name: a_cols minus past_panels times the transpose of the top 1024 rows of past_panels is the first 1024 columns of a symmetric positive definite matrix whose top block has eigenvalues between 2 and 12.
All inputs are finite; a program needn't handle non-finite values.
Results may differ from the reference program's by a relative error of at most 0.0001.
Values sent between devices are 32-bit elements.
A program may use at most 64 MiB of HBM per device.

```python
import math
import jax
import jax.numpy as jnp
from jax import lax

NB = 512
STEPS = 2
ROWS = 4096
W = 1024
PAST = 2048


def shared_draw(key):
    spread = jnp.sqrt(jnp.float32(0.4) / PAST)
    past = jnp.clip(jax.random.normal(jax.random.fold_in(key, 11), (ROWS, PAST), jnp.float32), -5.0, 5.0) * spread
    basis = jnp.clip(jax.random.normal(jax.random.fold_in(key, 12), (ROWS, W), jnp.float32), -5.0, 5.0)
    extra = jnp.exp(jax.random.uniform(jax.random.fold_in(key, 13), (W,), jnp.float32, math.log(2.0), math.log(4.0)))
    dims = (((1,), (1,)), ((), ()))
    schur = lax.dot_general(basis, basis[:W], dims, precision=lax.Precision.HIGHEST, preferred_element_type=jnp.float32) / W
    schur = schur.at[:W].add(jnp.diag(extra))
    whole = lax.dot_general(past, past[:W], dims, precision=lax.Precision.HIGHEST, preferred_element_type=jnp.float32) + schur
    return (whole, past)


def draw_a_cols(key, part):
    return shared_draw(key)[0]


def draw_past_panels(key, part):
    return shared_draw(key)[1]


def setup_inputs(seed: int = 0) -> dict:
    key_of = jax.random.split(jax.random.key(seed), 3)
    a_cols = draw_a_cols(jax.random.fold_in(key_of[2], 71), 0)
    past_panels = draw_past_panels(jax.random.fold_in(key_of[2], 71), 0)
    return {"a_cols": a_cols, "past_panels": past_panels}


def outer_rows(left, right):
    return lax.dot_general(left.astype(jnp.float32), right.astype(jnp.float32), (((1,), (1,)), ((), ())), precision=lax.Precision.HIGHEST, preferred_element_type=jnp.float32)

def reference(a_cols, past_panels):
    result = jnp.zeros((ROWS, W), jnp.float32)
    row_ids = jnp.arange(ROWS, dtype=jnp.int32)[:, None]
    col_ids = jnp.arange(NB, dtype=jnp.int32)[None, :]
    for section in range(STEPS):
        start = section * NB
        summed = outer_rows(past_panels, past_panels[start:start + NB])
        if section > 0:
            summed = summed + outer_rows(result[:, :start], result[start:start + NB, :start])
        update = a_cols[:, start:start + NB] - summed
        diag_factor = jnp.linalg.cholesky(update[start:start + NB])
        solved = jax.scipy.linalg.solve_triangular(diag_factor, update.T, lower=True).T
        new_panel = jnp.where(row_ids >= start + col_ids, solved, jnp.float32(0.0))
        result = result.at[:, start:start + NB].set(new_panel)
    return result
```

```python
import functools

import jax
import jax.numpy as jnp
from jax import lax
from jax.experimental import pallas as pl
from jax.experimental.pallas import tpu as pltpu
from jax.sharding import PartitionSpec as P

MESH = pl.DeviceIdType.MESH
F32 = jnp.float32
BF16 = jnp.bfloat16
BLK = 256
SUB = 128
VMEM_LIMIT = 60 * 1024 * 1024
LOW, HIGH = 2.0, 12.0


def ring_next(r, n, flip):
    if n == 4:
        y, x = r // 2, r % 2
        return (1 - x) * 2 + y if flip else x * 2 + (1 - y)
    return lax.rem(r + n - 1, n) if flip else lax.rem(r + 1, n)


def at(row, col, depth):
    return {"row": row, "col": col, "depth": depth}


def greet(nrow, ncol, ndepth):
    row, col, dep = lax.axis_index("row"), lax.axis_index("col"), lax.axis_index("depth")
    barrier = pltpu.get_barrier_semaphore()
    count = 0
    for s in range(1, ndepth):
        pl.semaphore_signal(barrier, inc=1, device_id=at(row, col, lax.rem(dep + s, ndepth)), device_id_type=MESH)
        count += 1
    for s in range(1, ncol):
        pl.semaphore_signal(barrier, inc=1, device_id=at(row, lax.rem(col + s, ncol), dep), device_id_type=MESH)
        count += 1
    for s in range(1, nrow):
        pl.semaphore_signal(barrier, inc=1, device_id=at(lax.rem(row + s, nrow), col, dep), device_id_type=MESH)
        count += 1
    pl.semaphore_wait(barrier, count)


def gather_kernel(nrow, ncol, ndepth, chunks, own, top, ring_send, ring_recv, side_send, side_recv0, side_recv1):
    greet(nrow, ncol, ndepth)
    spread_all(nrow, ncol, own, top, (own.shape[1],) * 2, chunks, (ring_send, ring_recv, side_send, (side_recv0, side_recv1)))


def spread_all(nrow, ncol, own, top, widths, chunks, sems, ready=None):
    row, col, dep = lax.axis_index("row"), lax.axis_index("col"), lax.axis_index("depth")
    ring_send, ring_recv, side_send, side_recv = sems
    size = own.shape[0] // chunks

    def part(ref, k, half, width):
        return ref.at[pl.ds(k * size, size), pl.ds(half * (width // 2), width // 2)]

    for owner in range(2):
        width = widths[owner]
        held = top.at[owner]

        def hop(k, half, src):
            return pltpu.make_async_remote_copy(
                src_ref=part(src, k, half, width), dst_ref=part(held, k, half, width),
                send_sem=ring_send.at[half, k], recv_sem=ring_recv.at[half, k],
                device_id=at(ring_next(row, nrow, half == 1), col, dep), device_id_type=MESH)

        def side(s, k, half, src):
            return pltpu.make_async_remote_copy(
                src_ref=part(src, k, half, width), dst_ref=part(held, k, half, width),
                send_sem=side_send.at[s - 1, half, k], recv_sem=side_recv[owner].at[half, k],
                device_id=at(row, lax.rem(col + s, ncol), dep), device_id_type=MESH)

        def goes_on(half):
            return ring_next(row, nrow, half == 1) != 0

        @pl.when(jnp.logical_and(col == owner, row == 0))
        def _():
            for k in range(chunks):
                if ready is not None:
                    ready(k)
                for half in range(2):
                    hop(k, half, own).start()
                    for s in range(1, ncol):
                        side(s, k, half, own).start()
            for k in range(chunks):
                for half in range(2):
                    hop(k, half, own).wait_send()
                    for s in range(1, ncol):
                        side(s, k, half, own).wait_send()
            held[:, pl.ds(0, width)] = own[:, pl.ds(0, width)]

        @pl.when(jnp.logical_and(col == owner, row != 0))
        def _():
            for k in range(chunks):
                for half in range(2):
                    hop(k, half, held).wait_recv()

                    @pl.when(goes_on(half))
                    def _():
                        hop(k, half, held).start()
                    for s in range(1, ncol):
                        side(s, k, half, held).start()
            for k in range(chunks):
                for half in range(2):
                    @pl.when(goes_on(half))
                    def _():
                        hop(k, half, held).wait_send()
                    for s in range(1, ncol):
                        side(s, k, half, held).wait_send()

        @pl.when(col != owner)
        def _():
            for k in range(chunks):
                for half in range(2):
                    side(1, k, half, held).wait_recv()


def reduce_kernel(nrow, ncol, ndepth, widths, part_ref, a_ref, own, top,
                  got, rs_send, rs_recv, ag_send, ag_recv, ring_send, ring_recv, side_send, side_recv0, side_recv1):
    row, col, dep = lax.axis_index("row"), lax.axis_index("col"), lax.axis_index("depth")
    size = own.shape[0] // ndepth
    greet(nrow, ncol, ndepth)

    def rows(index):
        return pl.ds(pl.multiple_of(index * size, size), size)

    def scatter(s):
        other = lax.rem(dep + s, ndepth)
        return pltpu.make_async_remote_copy(
            src_ref=part_ref.at[rows(other)], dst_ref=got.at[s - 1],
            send_sem=rs_send.at[s - 1], recv_sem=rs_recv.at[s - 1],
            device_id=at(row, col, other), device_id_type=MESH)

    def share(s):
        return pltpu.make_async_remote_copy(
            src_ref=own.at[rows(dep)], dst_ref=own.at[rows(dep)],
            send_sem=ag_send.at[s - 1], recv_sem=ag_recv.at[s - 1],
            device_id=at(row, col, lax.rem(dep + s, ndepth)), device_id_type=MESH)

    for s in range(1, ndepth):
        scatter(s).start()
    total = part_ref[rows(dep), :]
    for s in range(1, ndepth):
        scatter(s).wait_recv()
        total = total + got[s - 1]
    own[rows(dep), :] = a_ref[rows(dep), :] - total
    for s in range(1, ndepth):
        share(s).start()
    for s in range(1, ndepth):
        other = lax.rem(dep + ndepth - s, ndepth)
        pltpu.make_async_remote_copy(
            src_ref=own.at[rows(other)], dst_ref=own.at[rows(other)],
            send_sem=ag_send.at[s - 1], recv_sem=ag_recv.at[s - 1],
            device_id=at(row, col, other), device_id_type=MESH).wait_recv()
    for s in range(1, ndepth):
        scatter(s).wait_send()
        share(s).wait_send()
    spread_all(nrow, ncol, own, top, widths, ndepth, (ring_send, ring_recv, side_send, (side_recv0, side_recv1)))


def split(x):
    high = x.astype(BF16)
    return high, (x - high.astype(F32)).astype(BF16)


NN = (((1,), (0,)), ((), ()))
NT = (((1,), (1,)), ((), ()))
TN = (((0,), (0,)), ((), ()))


def dot1(x, y, dims):
    return lax.dot_general(x, y, dims, preferred_element_type=F32)


def dot3(x, y, dims):
    (xh, xl), (yh, yl) = x, y
    return dot1(xh, yh, dims) + (dot1(xh, yl, dims) + dot1(xl, yh, dims))


def eye(n):
    return (lax.broadcasted_iota(jnp.int32, (n, n), 0) == lax.broadcasted_iota(jnp.int32, (n, n), 1)).astype(F32)


def inverses(blocks):
    unit = eye(blocks[0].shape[0])
    mid, rad = (HIGH + LOW) / 2, (HIGH - LOW) / 2
    t2 = 2 * (mid / rad) ** 2 - 1
    c1, c2 = 4 * mid / (rad * rad * t2), -2 / (rad * rad * t2)
    xs = [c1 * unit + c2 * b for b in blocks]
    halves = [split(b) for b in blocks]
    for step in range(5):
        if step < 2:
            xs = [x.astype(BF16).astype(F32) for x in xs]
            es = [unit - dot1(h[0], x.astype(BF16), NN) for h, x in zip(halves, xs)]
            xs = [x + dot1(x.astype(BF16), e.astype(BF16), NN) for x, e in zip(xs, es)]
        else:
            ss = [split(x) for x in xs]
            es = [unit - dot3(h, s, NN) for h, s in zip(halves, ss)]
            xs = [x + dot1(s[0], e.astype(BF16), NN) if step == 4 else x + dot3(s, split(e), NN)
                  for x, s, e in zip(xs, ss, es)]
    return xs


def base_cholesky(mats, n, count):
    sub = lax.broadcasted_iota(jnp.int32, (count, 8, n), 1)
    lane = lax.broadcasted_iota(jnp.int32, (count, 8, n), 2)
    for j in range(n // 8):
        r = mats[:, 8 * j:8 * j + 8, :]
        for t in range(8):
            c = 8 * j + t
            column = r[:, :, c:c + 1]
            d = column[:, t:t + 1, :]
            inv = lax.rsqrt(d)
            inv = inv * (1.5 - 0.5 * d * inv * inv)
            u = r[:, t:t + 1, :] * inv
            r = jnp.where(sub > t, r - (column * inv) * u, jnp.where(sub == t, u, r))
        r = jnp.where(lane >= sub + 8 * j, r, 0.0)
        mats[:, 8 * j:8 * j + 8, :] = r
        if j + 1 < n // 8:
            high = r.astype(BF16).astype(F32)
            low = r - high
            left = jnp.concatenate([high, high, low], axis=1).astype(BF16)
            right = jnp.concatenate([high, low, high], axis=1).astype(BF16)
            start = 8 * (j + 1)
            for b in range(count):
                out = dot1(left[b], right[b], TN)
                mats[b, start:, :] = mats[b, start:, :] - out[start:, :]


def factor_kernel(own_ref, top_ref, out_ref, work, mh, ml, uh, ul, mats, inner):
    nb, width = top_ref.shape[1], own_ref.shape[1]
    rows = own_ref.shape[0]
    for half in range(2):
        work[half * nb:(half + 1) * nb, :(half + 1) * nb] = top_ref[half, :, :(half + 1) * nb]
    work[width:width + rows, :] = own_ref[...]
    steps = width // BLK
    for k in range(steps):
        lo, hi = k * BLK, (k + 1) * BLK
        if k > 0:
            right = (uh[lo:hi, :lo], ul[lo:hi, :lo])
            for r in range(lo, width + rows, BLK):
                left = (mh[r:r + BLK, :lo], ml[r:r + BLK, :lo])
                work[r:r + BLK, lo:hi] = work[r:r + BLK, lo:hi] - dot3(left, right, NT)
        inv = split(inverses([work[lo:hi, lo:hi]])[0])
        for r in range(hi, width + rows, BLK):
            u = split(work[r:r + BLK, lo:hi])
            uh[r:r + BLK, lo:hi], ul[r:r + BLK, lo:hi] = u
            m = dot3(u, inv, NN)
            mh[r:r + BLK, lo:hi], ml[r:r + BLK, lo:hi] = split(m)
    diag = [work[k * BLK:(k + 1) * BLK, k * BLK:(k + 1) * BLK] for k in range(steps)]
    invs = inverses([d[:SUB, :SUB] for d in diag])
    for k in range(steps):
        lo, mid, hi = k * BLK, k * BLK + SUB, (k + 1) * BLK
        low = split(work[mid:hi, lo:mid])
        m = split(dot3(low, split(invs[k]), NN))
        inner[k] = m[0].astype(F32) + m[1].astype(F32)
        mats[2 * k] = work[lo:mid, lo:mid]
        mats[2 * k + 1] = work[mid:hi, mid:hi] - dot3(m, low, NT)
    base_cholesky(mats, SUB, 2 * steps)
    position = lax.axis_index("row") * lax.axis_size("col") + lax.axis_index("col")
    first = position * rows
    for k in range(steps):
        lo, mid, hi = k * BLK, k * BLK + SUB, (k + 1) * BLK
        t1, t2 = split(mats[2 * k]), split(mats[2 * k + 1])
        l21 = split(dot3(split(inner[k]), t1, NT))
        for r in range(0, rows, BLK):
            w = width + r
            p1 = (mh[w:w + BLK, lo:mid], ml[w:w + BLK, lo:mid])
            p2 = (mh[w:w + BLK, mid:hi], ml[w:w + BLK, mid:hi])
            x1 = dot3(p1, t1, NT) + dot3(p2, l21, NN)
            x2 = dot3(p2, t2, NT)
            ids = first + r + lax.broadcasted_iota(jnp.int32, (BLK, SUB), 0)
            cols = lax.broadcasted_iota(jnp.int32, (BLK, SUB), 1)
            out_ref[r:r + BLK, lo:mid] = jnp.where(ids >= lo + cols, x1, 0.0)
            out_ref[r:r + BLK, mid:hi] = jnp.where(ids >= mid + cols, x2, 0.0)


def vmem(n):
    return [pl.BlockSpec(memory_space=pltpu.VMEM)] * n


def spread_sems(ncol, chunks):
    dma = pltpu.SemaphoreType.DMA
    return [dma((2, chunks)), dma((2, chunks)), dma((ncol - 1, 2, chunks)), dma((2, chunks)), dma((2, chunks))]


def solution(mesh):
    nrow, ncol, ndepth = (mesh.shape[name] for name in ("row", "col", "depth"))
    chunks = 4

    def body(a_cols, past_panels):
        rows, width = a_cols.shape
        past = past_panels.shape[1]
        top = pl.pallas_call(
            functools.partial(gather_kernel, nrow, ncol, ndepth, chunks),
            out_shape=jax.ShapeDtypeStruct((2, rows, past), F32),
            in_specs=vmem(1), out_specs=vmem(1)[0],
            scratch_shapes=spread_sems(ncol, chunks),
            compiler_params=pltpu.CompilerParams(collective_id=0, has_side_effects=True),
        )(past_panels)
        partial = lax.dot_general(past_panels, top.reshape(2 * rows, past), NT,
                                  precision=lax.Precision.HIGH, preferred_element_type=F32)
        dma = pltpu.SemaphoreType.DMA
        own, head = pl.pallas_call(
            functools.partial(reduce_kernel, nrow, ncol, ndepth, (rows, 2 * rows)),
            out_shape=[jax.ShapeDtypeStruct((rows, width), F32), jax.ShapeDtypeStruct((2, rows, width), F32)],
            in_specs=vmem(2), out_specs=vmem(2),
            scratch_shapes=[pltpu.VMEM((ndepth - 1, rows // ndepth, width), F32)]
            + [dma((ndepth - 1,))] * 4 + spread_sems(ncol, ndepth),
            compiler_params=pltpu.CompilerParams(collective_id=1, has_side_effects=True, vmem_limit_bytes=VMEM_LIMIT),
        )(partial, a_cols)
        halves = [pltpu.VMEM((width + rows, width), BF16)] * 4
        return pl.pallas_call(
            factor_kernel,
            out_shape=jax.ShapeDtypeStruct((rows, width), F32),
            in_specs=vmem(2), out_specs=vmem(1)[0],
            scratch_shapes=[pltpu.VMEM((width + rows, width), F32)] + halves
            + [pltpu.VMEM((width // SUB, SUB, SUB), F32), pltpu.VMEM((width // BLK, SUB, SUB), F32)],
            compiler_params=pltpu.CompilerParams(vmem_limit_bytes=VMEM_LIMIT),
        )(own, head)

    in_specs = (P(("row", "col"), None), P(("row", "col"), "depth"))
    out_specs = P(("row", "col"), None)
    return jax.shard_map(body, mesh=mesh, in_specs=in_specs, out_specs=out_specs, check_vma=False)
```

```python
import functools

import jax
import jax.numpy as jnp
from jax import lax
from jax.experimental import pallas as pl
from jax.experimental.pallas import tpu as pltpu
from jax.sharding import PartitionSpec as P

MESH = pl.DeviceIdType.MESH
F32 = jnp.float32
BF16 = jnp.bfloat16
BLK = 256
SUB = 128
VMEM_LIMIT = 60 * 1024 * 1024
LOW, HIGH = 2.0, 12.0


def ring_next(r, n, flip):
    return tour(r, n, flip)


def tour(r, n, flip):
    if n == 4:
        y, x = r // 2, r % 2
        return (1 - x) * 2 + y if flip else x * 2 + (1 - y)
    return (r + n - 1) % n if flip else (r + 1) % n


def at(row, col, depth):
    return {"row": row, "col": col, "depth": depth}


def greet(nrow, ncol, ndepth):
    row, col, dep = lax.axis_index("row"), lax.axis_index("col"), lax.axis_index("depth")
    barrier = pltpu.get_barrier_semaphore()
    count = 0
    for s in range(1, ndepth):
        pl.semaphore_signal(barrier, inc=1, device_id=at(row, col, lax.rem(dep + s, ndepth)), device_id_type=MESH)
        count += 1
    for s in range(1, ncol):
        pl.semaphore_signal(barrier, inc=1, device_id=at(row, lax.rem(col + s, ncol), dep), device_id_type=MESH)
        count += 1
    for s in range(1, nrow):
        pl.semaphore_signal(barrier, inc=1, device_id=at(lax.rem(row + s, nrow), col, dep), device_id_type=MESH)
        count += 1
    pl.semaphore_wait(barrier, count)


def gather_kernel(nrow, ncol, ndepth, chunks, own, top, *sems):
    greet(nrow, ncol, ndepth)
    order = list(range(chunks))
    spread(nrow, ncol, own, top, (own.shape[1],) * 2, own.shape[0] // chunks, order, sems)


def arrivals(r, n, chunks):
    tours = []
    for half in range(2):
        place, hops = 0, 0
        while place != r:
            place, hops = int(tour(place, n, half == 1)), hops + 1
        tours.append(hops)
    events = [(k + tours[half], half, k) for k in range(chunks) for half in range(2)]
    return [(k, half) for _, half, k in sorted(events)]


def spread(nrow, ncol, own, top, widths, size, order, sems, ready=None):
    row, col, dep = lax.axis_index("row"), lax.axis_index("col"), lax.axis_index("depth")
    ring_send, ring_recv, side_send, *side_recv = sems
    chunks = len(order)

    def part(ref, k, half, width):
        slab = order[k] * size if isinstance(order[k], int) else pl.multiple_of(order[k] * size, size)
        return ref.at[pl.ds(slab, size), pl.ds(half * (width // 2), width // 2)]

    def hop(owner, k, half, src):
        return pltpu.make_async_remote_copy(
            src_ref=part(src, k, half, widths[owner]), dst_ref=part(top.at[owner], k, half, widths[owner]),
            send_sem=ring_send.at[half, k], recv_sem=ring_recv.at[half, k],
            device_id=at(ring_next(row, nrow, half == 1), col, dep), device_id_type=MESH)

    def side(owner, s, k, half, src):
        return pltpu.make_async_remote_copy(
            src_ref=part(src, k, half, widths[owner]), dst_ref=part(top.at[owner], k, half, widths[owner]),
            send_sem=side_send.at[s - 1, half, k], recv_sem=side_recv[owner].at[half, k],
            device_id=at(row, lax.rem(col + s, ncol), dep), device_id_type=MESH)

    for owner in range(2):
        held = top.at[owner]
        for r in range(nrow):
            src = own if r == 0 else held

            @pl.when(jnp.logical_and(col == owner, row == r))
            def _():
                seen = -1
                events = [(k, half) for k in range(chunks) for half in range(2)] if r == 0 else arrivals(r, nrow, chunks)
                last = [r != 0 and int(tour(r, nrow, half == 1)) == 0 for half in range(2)]
                for k, half in events:
                    if r != 0:
                        hop(owner, k, half, held).wait_recv()
                    elif ready is not None and k > seen:
                        ready(k)
                        seen = k
                    if not last[half]:
                        hop(owner, k, half, src).start()
                    for s in range(1, ncol):
                        side(owner, s, k, half, src).start()
                if r == 0:
                    held[:, pl.ds(0, widths[owner])] = own[:, pl.ds(0, widths[owner])]
                for k, half in events:
                    if not last[half]:
                        hop(owner, k, half, src).wait_send()
                    for s in range(1, ncol):
                        side(owner, s, k, half, src).wait_send()

    for owner in range(2):
        @pl.when(col != owner)
        def _():
            for k in range(chunks):
                for half in range(2):
                    side(owner, 1, k, half, top.at[owner]).wait_recv()


def reduce_kernel(nrow, ncol, ndepth, widths, part_ref, a_ref, own, top, got, rs_send, rs_recv, ag_send, ag_recv, *sems):
    row, col, dep = lax.axis_index("row"), lax.axis_index("col"), lax.axis_index("depth")
    size = own.shape[0] // ndepth
    greet(nrow, ncol, ndepth)

    def rows(index):
        return pl.ds(pl.multiple_of(index * size, size), size)

    def scatter(s):
        other = lax.rem(dep + s, ndepth)
        return pltpu.make_async_remote_copy(
            src_ref=part_ref.at[rows(other)], dst_ref=got.at[s - 1],
            send_sem=rs_send.at[s - 1], recv_sem=rs_recv.at[s - 1],
            device_id=at(row, col, other), device_id_type=MESH)

    def share(s):
        return pltpu.make_async_remote_copy(
            src_ref=own.at[rows(dep)], dst_ref=own.at[rows(dep)],
            send_sem=ag_send.at[s - 1], recv_sem=ag_recv.at[s - 1],
            device_id=at(row, col, lax.rem(dep + s, ndepth)), device_id_type=MESH)

    def arrived(s):
        other = lax.rem(dep + ndepth - s, ndepth)
        pltpu.make_async_remote_copy(
            src_ref=own.at[rows(other)], dst_ref=own.at[rows(other)],
            send_sem=ag_send.at[s - 1], recv_sem=ag_recv.at[s - 1],
            device_id=at(row, col, other), device_id_type=MESH).wait_recv()

    for s in range(1, ndepth):
        scatter(s).start()
    total = part_ref[rows(dep), :]
    for s in range(1, ndepth):
        scatter(s).wait_recv()
        total = total + got[s - 1]
    own[rows(dep), :] = a_ref[rows(dep), :] - total
    for s in range(1, ndepth):
        share(s).start()
    order = [lax.rem(dep + ndepth - s, ndepth) for s in range(ndepth)]
    spread(nrow, ncol, own, top, widths, size, order, sems, ready=lambda s: arrived(s) if s else None)

    @pl.when(jnp.logical_or(row != 0, col >= 2))
    def _():
        for s in range(1, ndepth):
            arrived(s)
    for s in range(1, ndepth):
        scatter(s).wait_send()
        share(s).wait_send()


def split(x):
    high = x.astype(BF16)
    return high, (x - high.astype(F32)).astype(BF16)


NN = (((1,), (0,)), ((), ()))
NT = (((1,), (1,)), ((), ()))
TN = (((0,), (0,)), ((), ()))


def dot1(x, y, dims):
    return lax.dot_general(x, y, dims, preferred_element_type=F32)


def dot3(x, y, dims):
    (xh, xl), (yh, yl) = x, y
    return dot1(xh, yh, dims) + (dot1(xh, yl, dims) + dot1(xl, yh, dims))


def eye(n):
    return (lax.broadcasted_iota(jnp.int32, (n, n), 0) == lax.broadcasted_iota(jnp.int32, (n, n), 1)).astype(F32)


def inverses(blocks):
    unit = eye(blocks[0].shape[0])
    mid, rad = (HIGH + LOW) / 2, (HIGH - LOW) / 2
    t2 = 2 * (mid / rad) ** 2 - 1
    c1, c2 = 4 * mid / (rad * rad * t2), -2 / (rad * rad * t2)
    xs = [c1 * unit + c2 * b for b in blocks]
    halves = [split(b) for b in blocks]
    for step in range(5):
        if step < 2:
            xs = [x.astype(BF16).astype(F32) for x in xs]
            es = [unit - dot1(h[0], x.astype(BF16), NN) for h, x in zip(halves, xs)]
            xs = [x + dot1(x.astype(BF16), e.astype(BF16), NN) for x, e in zip(xs, es)]
        else:
            ss = [split(x) for x in xs]
            es = [unit - dot3(h, s, NN) for h, s in zip(halves, ss)]
            xs = [x + dot1(s[0], e.astype(BF16), NN) if step == 4 else x + dot3(s, split(e), NN)
                  for x, s, e in zip(xs, ss, es)]
    return xs


def base_cholesky(mats, n, count):
    sub = lax.broadcasted_iota(jnp.int32, (count, 8, n), 1)
    lane = lax.broadcasted_iota(jnp.int32, (count, 8, n), 2)
    for j in range(n // 8):
        r = mats[:, 8 * j:8 * j + 8, :]
        for t in range(8):
            c = 8 * j + t
            column = r[:, :, c:c + 1]
            d = column[:, t:t + 1, :]
            inv = lax.rsqrt(d)
            inv = inv * (1.5 - 0.5 * d * inv * inv)
            u = r[:, t:t + 1, :] * inv
            r = jnp.where(sub > t, r - (column * inv) * u, jnp.where(sub == t, u, r))
        r = jnp.where(lane >= sub + 8 * j, r, 0.0)
        mats[:, 8 * j:8 * j + 8, :] = r
        if j + 1 < n // 8:
            high = r.astype(BF16).astype(F32)
            low = r - high
            left = jnp.concatenate([high, high, low], axis=1).astype(BF16)
            right = jnp.concatenate([high, low, high], axis=1).astype(BF16)
            start = 8 * (j + 1)
            for b in range(count):
                out = dot1(left[b], right[b], TN)
                mats[b, start:, :] = mats[b, start:, :] - out[start:, :]


def factor_kernel(own_ref, top_ref, out_ref, work, mh, ml, uh, ul, mats, inner):
    nb, width = top_ref.shape[1], own_ref.shape[1]
    rows = own_ref.shape[0]
    for half in range(2):
        work[half * nb:(half + 1) * nb, :(half + 1) * nb] = top_ref[half, :, :(half + 1) * nb]
    work[width:width + rows, :] = own_ref[...]
    steps = width // BLK
    for k in range(steps):
        lo, hi = k * BLK, (k + 1) * BLK
        if k > 0:
            right = (uh[lo:hi, :lo], ul[lo:hi, :lo])
            for r in range(lo, width + rows, BLK):
                left = (mh[r:r + BLK, :lo], ml[r:r + BLK, :lo])
                work[r:r + BLK, lo:hi] = work[r:r + BLK, lo:hi] - dot3(left, right, NT)
        inv = split(inverses([work[lo:hi, lo:hi]])[0])
        for r in range(hi, width + rows, BLK):
            u = split(work[r:r + BLK, lo:hi])
            uh[r:r + BLK, lo:hi], ul[r:r + BLK, lo:hi] = u
            m = dot3(u, inv, NN)
            mh[r:r + BLK, lo:hi], ml[r:r + BLK, lo:hi] = split(m)
    diag = [work[k * BLK:(k + 1) * BLK, k * BLK:(k + 1) * BLK] for k in range(steps)]
    invs = inverses([d[:SUB, :SUB] for d in diag])
    for k in range(steps):
        lo, mid, hi = k * BLK, k * BLK + SUB, (k + 1) * BLK
        low = split(work[mid:hi, lo:mid])
        m = split(dot3(low, split(invs[k]), NN))
        inner[k] = m[0].astype(F32) + m[1].astype(F32)
        mats[2 * k] = work[lo:mid, lo:mid]
        mats[2 * k + 1] = work[mid:hi, mid:hi] - dot3(m, low, NT)
    base_cholesky(mats, SUB, 2 * steps)
    position = lax.axis_index("row") * lax.axis_size("col") + lax.axis_index("col")
    first = position * rows
    for k in range(steps):
        lo, mid, hi = k * BLK, k * BLK + SUB, (k + 1) * BLK
        t1, t2 = split(mats[2 * k]), split(mats[2 * k + 1])
        l21 = split(dot3(split(inner[k]), t1, NT))
        for r in range(0, rows, BLK):
            w = width + r
            p1 = (mh[w:w + BLK, lo:mid], ml[w:w + BLK, lo:mid])
            p2 = (mh[w:w + BLK, mid:hi], ml[w:w + BLK, mid:hi])
            x1 = dot3(p1, t1, NT) + dot3(p2, l21, NN)
            x2 = dot3(p2, t2, NT)
            ids = first + r + lax.broadcasted_iota(jnp.int32, (BLK, SUB), 0)
            cols = lax.broadcasted_iota(jnp.int32, (BLK, SUB), 1)
            out_ref[r:r + BLK, lo:mid] = jnp.where(ids >= lo + cols, x1, 0.0)
            out_ref[r:r + BLK, mid:hi] = jnp.where(ids >= mid + cols, x2, 0.0)


def vmem(n):
    return [pl.BlockSpec(memory_space=pltpu.VMEM)] * n


def spread_sems(ncol, chunks):
    dma = pltpu.SemaphoreType.DMA
    return [dma((2, chunks)), dma((2, chunks)), dma((ncol - 1, 2, chunks)), dma((2, chunks)), dma((2, chunks))]


def solution(mesh):
    nrow, ncol, ndepth = (mesh.shape[name] for name in ("row", "col", "depth"))
    chunks = 4

    def body(a_cols, past_panels):
        rows, width = a_cols.shape
        past = past_panels.shape[1]
        top = pl.pallas_call(
            functools.partial(gather_kernel, nrow, ncol, ndepth, chunks),
            out_shape=jax.ShapeDtypeStruct((2, rows, past), F32),
            in_specs=vmem(1), out_specs=vmem(1)[0],
            scratch_shapes=spread_sems(ncol, chunks),
            compiler_params=pltpu.CompilerParams(collective_id=0, has_side_effects=True),
        )(past_panels)
        partial = lax.dot_general(past_panels, top.reshape(2 * rows, past), NT,
                                  precision=lax.Precision.HIGH, preferred_element_type=F32)
        dma = pltpu.SemaphoreType.DMA
        own, head = pl.pallas_call(
            functools.partial(reduce_kernel, nrow, ncol, ndepth, (rows, 2 * rows)),
            out_shape=[jax.ShapeDtypeStruct((rows, width), F32), jax.ShapeDtypeStruct((2, rows, width), F32)],
            in_specs=vmem(2), out_specs=vmem(2),
            scratch_shapes=[pltpu.VMEM((ndepth - 1, rows // ndepth, width), F32)]
            + [dma((ndepth - 1,))] * 4 + spread_sems(ncol, ndepth),
            compiler_params=pltpu.CompilerParams(collective_id=1, has_side_effects=True, vmem_limit_bytes=VMEM_LIMIT),
        )(partial, a_cols)
        halves = [pltpu.VMEM((width + rows, width), BF16)] * 4
        return pl.pallas_call(
            factor_kernel,
            out_shape=jax.ShapeDtypeStruct((rows, width), F32),
            in_specs=vmem(2), out_specs=vmem(1)[0],
            scratch_shapes=[pltpu.VMEM((width + rows, width), F32)] + halves
            + [pltpu.VMEM((width // SUB, SUB, SUB), F32), pltpu.VMEM((width // BLK, SUB, SUB), F32)],
            compiler_params=pltpu.CompilerParams(vmem_limit_bytes=VMEM_LIMIT),
        )(own, head)

    in_specs = (P(("row", "col"), None), P(("row", "col"), "depth"))
    out_specs = P(("row", "col"), None)
    return jax.shard_map(body, mesh=mesh, in_specs=in_specs, out_specs=out_specs, check_vma=False)
```
